32 devices in a mesh: expert: 4 (over z), panel: 8 (over y, x, core).
Axes of the slice: x: 2, y: 2, z: 4, core: 2. Of those that a mesh axis runs over, the one named last changes fastest.
Arguments:
- tokens: bfloat16 [1024, 6144], P(('expert', 'panel')), may hold values from -6 to 6
- routes: int32 [1024, 2], P(('expert', 'panel')), may hold values from 0 to 7, all different within a row; in each aligned block of 32 rows (0 to 31, 32 to 63, ...) at most 12 rows name the same one
- router_weights: float32 [1024, 2], P(('expert', 'panel')), may hold values from 0.05 to 0.95
Outputs:
- hessian: float32 [8, 6144, 6144], P('expert', 'panel')
The draws below stay inside these ranges and needn't reach their ends.
Inputs may be any that keep to these rules, and one draw needn't show every extreme that they name: `routes`: each row names two different experts; among the 32 rows of one device no expert is named more than 12 times, a bound that some block reaches.
All inputs are finite; a program needn't handle non-finite values.
Results may differ from the reference program's by a relative error of at most 0.0036.
Values may be sent and summed in bfloat16 or wider, within the bound.
No kernel may reach another device: no remote copies, remote signals or barrier semaphores. Data moves between devices by JAX's collectives and lax.ppermute only.
A program may use at most 192 MiB of HBM per device.

```python
import math
import jax
import jax.numpy as jnp
import numpy as np
from jax import lax

D = 6144
TOK_DEV = 32
CAP = 12
EXPERTS = 8
TOKENS = 1024
N_EXPERT = 4
N_PANEL = 8


def steps_of(own_key, shape, cuts, low, high):
    factor_of, own = 1.0, jax.random.fold_in(own_key, 6)
    for position, parts in cuts:
        draws = jnp.exp(jax.random.uniform(jax.random.fold_in(own, position), (parts,), jnp.float32, low / len(cuts), high / len(cuts)))
        factor_of = factor_of * jnp.repeat(draws, shape[position] // parts).reshape([-1 if axis == position else 1 for axis in range(len(shape))])
    return factor_of


def assign_block(rng, own, number, rows, amount, top, reach, lean):
    order = jax.random.permutation(rng, amount)
    packed, common = shares(amount, rows * top, reach, lean, True), shares(amount, rows * top, reach, lean, False)
    places = jnp.arange(amount)

    def named(sizes, rotation):
        used = int((sizes > 0).sum())
        fixed = max(1, used // 4)
        moved = fixed + (places - fixed + rotation * (used - fixed)) % max(1, amount - fixed)
        return jnp.zeros((amount,), jnp.int32).at[order[jnp.where(places < fixed, places, moved)]].set(jnp.asarray(sizes, jnp.int32))

    sizes = jnp.where(number % 4 == 0, named(packed, number // 4), named(common, number - number // 4 - 1))
    mixed = jax.random.permutation(jax.random.fold_in(own, 3), amount)
    giver, taker = mixed[0:amount // 2 * 2:2], mixed[1:amount // 2 * 2:2]
    margin = jnp.minimum(sizes[giver] - 1, reach - sizes[taker]) // 2
    margin = jnp.where((giver == order[0]) | (taker == order[0]) | (sizes[taker] == 0), 0, jnp.maximum(margin, 0))
    moved = jax.random.randint(jax.random.fold_in(own, 4), (amount // 2,), 0, 1 << 20) % (margin + 1)
    sizes = sizes.at[giver].add(-moved).at[taker].add(moved)
    labels = jnp.searchsorted(jnp.cumsum(sizes), jnp.arange(rows * top), side="right").astype(jnp.int32)
    table = labels.reshape(top, rows).T
    table = table[jax.random.permutation(jax.random.fold_in(own, 1), rows)]
    rotation = jax.random.randint(jax.random.fold_in(own, 2), (rows, 1), 0, top)
    return jnp.take_along_axis(table, (jnp.arange(top)[None, :] + rotation) % top, axis=1)


def shares(amount, total, bound, lean, full):
    loads = [(1 << 20) // math.isqrt(grade ** lean) + 1 for grade in range(1, amount + 1)]
    largest = bound if full else min(bound, max(-(-total // amount), total * loads[0] // sum(loads)))
    least = 1 if total - largest >= amount - 1 else 0
    holding, surplus = [largest] + [least] * (amount - 1), total - largest - least * (amount - 1)
    while surplus > 0:
        free = [i for i in range(1, amount) if holding[i] < largest] or [i for i in range(1, amount) if holding[i] < bound]
        pool, left = sum([loads[i] for i in free]), surplus
        for i in free:
            more = min(bound - holding[i], max(1, left * loads[i] // pool), surplus)
            holding[i] = holding[i] + more
            surplus = surplus - more
    return np.array(holding)


def scatter_about(own_key, shape, deviation, bound, split=(), kind=jnp.bfloat16):
    entries = deviation * jax.random.normal(own_key, shape, jnp.float32)
    if split:
        entries = entries * steps_of(own_key, shape, split, -0.22, 0.18)
    return jnp.clip(entries, -bound, bound).astype(kind)


def setup_inputs(seed: int = 0) -> dict:
    seeds = jax.random.split(jax.random.key(seed), 4)
    tokens = scatter_about(seeds[0], (TOKENS, D), 1.0, 6.0, ((0, 32),))
    routes_keys = jax.random.split(jax.random.fold_in(seeds[1], 1), TOKENS // TOK_DEV)
    routes_turns = jax.random.permutation(jax.random.fold_in(seeds[1], 3), TOKENS // TOK_DEV)
    routes = jax.vmap(lambda own, number: assign_block(jax.random.fold_in(seeds[1], 2), own, number, TOK_DEV, EXPERTS, 2, CAP, 2))(routes_keys, routes_turns).reshape((TOKENS, 2))
    router_weights = jnp.clip(0.05 + 0.9 * jax.random.uniform(seeds[2], (TOKENS, 2), jnp.float32) ** steps_of(seeds[2], (TOKENS, 2), ((0, 32),), -0.2, 0.2), 0.05, 0.95)
    return dict(tokens=tokens, routes=routes, router_weights=router_weights)


def place_of(routes):
    blocks = routes.reshape(N_EXPERT * N_PANEL, TOK_DEV * 2)
    onehot = (blocks[:, :, None] == jnp.arange(EXPERTS, dtype=jnp.int32)).astype(jnp.int32)
    before = jnp.cumsum(onehot, axis=1) - onehot
    slots = jnp.sum(onehot * before, axis=2)
    device = jnp.arange(N_EXPERT * N_PANEL, dtype=jnp.int32)[:, None]
    return (device * CAP + slots).astype(jnp.int32).reshape(TOKENS, 2)


def reference(tokens, routes, router_weights):
    places = place_of(routes)
    rounded = lax.optimization_barrier(router_weights.astype(jnp.bfloat16)).astype(jnp.float32)
    widened = tokens.astype(jnp.float32)
    slot_total = N_EXPERT * N_PANEL * CAP
    scaling = float(slot_total) ** -0.5

    def one_expert(expert):
        chosen = routes == expert
        picked = jnp.any(chosen, axis=1)
        index = jnp.where(picked, jnp.sum(jnp.where(chosen, places, 0), axis=1), slot_total).astype(jnp.int32)
        factor = jnp.sum(jnp.where(chosen, rounded, 0.0), axis=1)
        scaled = lax.optimization_barrier((factor[:, None] * widened).astype(jnp.bfloat16)).astype(jnp.float32)
        plain = jnp.zeros((slot_total, D), jnp.float32).at[index].set(widened, mode="drop")
        weighted = jnp.zeros((slot_total, D), jnp.float32).at[index].set(scaled, mode="drop")
        return jnp.dot(plain.T, weighted, precision=lax.Precision.HIGHEST) * scaling

    return lax.map(one_expert, jnp.arange(EXPERTS, dtype=jnp.int32))
```

```python
import functools

import jax
import jax.numpy as jnp
from jax import lax
from jax.experimental import pallas as pl
from jax.experimental.pallas import tpu as pltpu
from jax.sharding import PartitionSpec as P


EXP_DEV = 2
CAP = 12
LANES = 128
MAX_VMEM = 28 * 1024 * 1024
SLOTS = 4
UNITS = (2, 2, 2)
FIRST = {"R": 0, "0": 1, "1": 0, "2": 1}
Z_GROUPS = ((0,), (1,), (2,))
STEPS = ((0,), (1, 2))


def flip(x, bit, count):
    return lax.ppermute(x, "panel", [(i, i ^ (1 << bit)) for i in range(count)])


def chunk_widths(panel_width):
    if panel_width % (LANES * sum(UNITS)):
        return [panel_width]
    return [panel_width // sum(UNITS) * u for u in UNITS]


def z_groups(widths):
    return Z_GROUPS if len(widths) > 1 else ((0,),)


def pick_kernel(groups, panels, widths, *refs):
    tok, tok_p, routes, routes_p, weights, weights_p = refs[:6]
    outs = refs[6:]
    rows = tok.shape[0]
    panel_width = sum(widths)
    core = lax.rem(lax.axis_index("panel"), EXP_DEV)
    z = lax.axis_index("expert")
    row = lax.broadcasted_iota(jnp.int32, (rows, rows), 0)
    col = lax.broadcasted_iota(jnp.int32, (rows, rows), 1)
    eye = (row == col).astype(jnp.float32)
    earlier = (row < col).astype(jnp.float32)
    slot = lax.broadcasted_iota(jnp.int32, (2 * CAP, rows), 0).astype(jnp.float32)

    def as_row(column):
        return jnp.sum(eye * column.astype(jnp.float32), axis=0, keepdims=True)

    pickers, factors = [], []
    halves = ((routes, weights), (routes_p, weights_p))
    lines = [[as_row(r[:, k : k + 1]) for k in (0, 1)] + [as_row(w[:, k : k + 1]) for k in (0, 1)] for r, w in halves]
    for shift in range(groups):
        expert = (EXP_DEV * (z ^ shift) + core).astype(jnp.float32)
        picks, factor = [], 0.0
        for half, (first, second, w_first, w_second) in enumerate(lines):
            is_first = (first == expert).astype(jnp.float32)
            is_second = (second == expert).astype(jnp.float32)
            member = is_first + is_second
            rank = jnp.dot(
                jnp.broadcast_to(member, (8, rows)), earlier, preferred_element_type=jnp.float32
            )[0:1]
            pick = (slot == rank + float(half * CAP)).astype(jnp.float32) * member
            factor = factor + jnp.sum(pick * (is_first * w_first + is_second * w_second), axis=1, keepdims=True)
            picks.append(pick)
        pickers.append(picks)
        factors.append(factor)
    own = jnp.concatenate([p[0] for p in pickers], axis=0).astype(jnp.bfloat16)
    other = jnp.concatenate([p[1] for p in pickers], axis=0).astype(jnp.bfloat16)
    slots = 2 * CAP
    start = 0
    for k, width in enumerate(widths):
        for q in range(panels):
            at = q * panel_width + start
            got = jnp.dot(own, tok[:, at : at + width], preferred_element_type=jnp.float32) + jnp.dot(
                other, tok_p[:, at : at + width], preferred_element_type=jnp.float32
            )
            got = got.astype(jnp.bfloat16)
            outs[0][:, start * panels + q * width : start * panels + (q + 1) * width] = got[:slots]
            for g, members in enumerate(z_groups(widths)):
                if k in members:
                    to = panels * sum(widths[j] for j in members if j < k) + q * width
                    for shift in range(1, groups):
                        outs[g * (groups - 1) + shift][:, to : to + width] = got[shift * slots : (shift + 1) * slots]
        start += width
    for shift in range(groups):
        at = outs[shift].shape[1] - LANES
        outs[shift][:, at:] = jnp.broadcast_to(factors[shift], (slots, LANES)).astype(jnp.bfloat16)


def anchor_kernel(x, y):
    y[...] = x[...]


def hessian_kernel(step, theirs, final, widths, panels, scaling, *refs):
    refs = list(refs)
    take = lambda n: [refs.pop(0) for _ in range(n)]
    common, parts = take(1)[0], take(len(STEPS[step]))
    old_scaled, old_panel = take(step), take(step)
    factor = take(1)[0] if step else None
    take(final + (step > 0 or theirs))
    out = take(1)[0]
    if not step:
        factor = take(1)[0]
    scaled, panel = take(2)
    tall, wide, sem = take(3)

    chunks, widths = widths, [sum(widths[k] for k in members) for members in STEPS]
    width, start = widths[step], sum(widths[:step])
    panel_width = sum(widths)
    index = lax.axis_index("panel")
    core = lax.rem(index, EXP_DEV)
    expert = 1 - core if theirs else core
    shared = common.shape[0]
    top, low = slice(0, shared), slice(shared, shared + parts[0].shape[0])
    if not step:
        factor[top] = common[:, panel_width * panels :]
        factor[low] = parts[0][:, panels * chunks[0] :]
    to = 0
    for k, part in zip(STEPS[step], parts):
        own = chunks[k]
        for at, ref, base in ((top, common, sum(chunks[:k]) * panels), (low, part, 0)):
            by = factor[at].astype(jnp.float32)
            for q in range(panels):
                for lane in range(0, own, LANES):
                    lanes = slice(base + q * own + lane, base + q * own + lane + LANES)
                    done = (ref[:, lanes].astype(jnp.float32) * by).astype(jnp.bfloat16)
                    scaled[at, q * width + to + lane : q * width + to + lane + LANES] = done
        columns = [ref[:, pl.ds(pl.multiple_of(base + index * own, LANES), own)] for ref, base in ((common, sum(chunks[:k]) * panels), (part, 0))]
        whole = jnp.concatenate([x.astype(jnp.float32) for x in columns], axis=0)
        panel[to : to + own, :] = whole.T.astype(jnp.bfloat16)
        to += own

    def copies(q):
        slot = lax.rem(q, SLOTS)
        at = pl.multiple_of(q * panel_width, LANES)
        made = [
            pltpu.make_async_copy(
                tall.at[slot],
                out.at[expert, pl.ds(0, start + width), pl.ds(pl.multiple_of(at + start, LANES), width)],
                sem.at[0, slot],
            )
        ]
        if step:
            made.append(
                pltpu.make_async_copy(
                    wide.at[slot],
                    out.at[expert, pl.ds(start, width), pl.ds(at, start)],
                    sem.at[1, slot],
                )
            )
        return made

    def body(q, carry):
        slot = lax.rem(q, SLOTS)

        @pl.when(q >= SLOTS)
        def _():
            for copy in copies(q - SLOTS):
                copy.wait()

        right = scaled[:, pl.ds(pl.multiple_of(q * width, LANES), width)]
        at = 0
        for j in range(step + 1):
            left = panel[...] if j == step else old_panel[j][...]
            tall[slot, at : at + widths[j], :] = jnp.dot(left, right, preferred_element_type=jnp.float32) * scaling
            at += widths[j]
        at = 0
        for j in range(step):
            right = old_scaled[j][:, pl.ds(pl.multiple_of(q * widths[j], LANES), widths[j])]
            wide[slot, :, at : at + widths[j]] = (
                jnp.dot(panel[...], right, preferred_element_type=jnp.float32) * scaling
            )
            at += widths[j]
        for copy in copies(q):
            copy.start()
        return carry

    lax.fori_loop(0, panels, body, 0)
    for q in range(panels - SLOTS, panels):
        for copy in copies(q):
            copy.wait()


def per_device(tokens, routes, router_weights):
    _, width = tokens.shape
    groups = lax.axis_size("expert")
    panels = lax.axis_size("panel")
    bits = panels.bit_length() - 1
    panel_width = width // panels
    scaling = float(groups * panels * CAP) ** (-0.5)
    slots = 2 * CAP
    widths = chunk_widths(panel_width)
    shapes = [(slots, width + LANES)]
    for g, members in enumerate(z_groups(widths)):
        shapes += [(slots, panels * sum(widths[k] for k in members) + LANES * (g == 0))] * (groups - 1)

    tok_p, routes_p, weights_p = (flip(x, 0, panels) for x in (tokens, routes, router_weights))
    vmem = pl.BlockSpec(memory_space=pltpu.VMEM)
    picked = pl.pallas_call(
        functools.partial(pick_kernel, groups, panels, widths),
        out_shape=[jax.ShapeDtypeStruct(x, jnp.bfloat16) for x in shapes],
        in_specs=[vmem] * 6,
        out_specs=[vmem] * len(shapes),
        compiler_params=pltpu.CompilerParams(vmem_limit_bytes=MAX_VMEM),
        name="pick",
    )(tokens, tok_p, routes, routes_p, router_weights, weights_p)

    def gather(k, piece):
        pieces = {0: piece}
        order = list(range(1, bits))
        turn = FIRST[k]
        for bit in order[turn:] + order[:turn]:
            more = {}
            for mask, piece in pieces.items():
                more[mask ^ (1 << bit)] = flip(piece, bit, panels)
            pieces |= more
        mine = jnp.concatenate([pieces[mask] for mask in sorted(pieces)], axis=0)
        return mine, flip(mine, 0, panels)

    held_all = gather("R", picked[0])
    held = []
    mark = jnp.zeros((8, LANES), jnp.float32)
    for g, members in enumerate(z_groups(widths)):
        came = []
        for shift in range(1, groups):
            sent = picked[1 + g * (groups - 1) + shift - 1]
            came.append(lax.ppermute(sent, "expert", [(i, i ^ shift) for i in range(groups)]))
        mark = pl.pallas_call(
            anchor_kernel,
            out_shape=jax.ShapeDtypeStruct(mark.shape, mark.dtype),
            in_specs=[vmem],
            out_specs=vmem,
            compiler_params=pltpu.CompilerParams(vmem_limit_bytes=MAX_VMEM),
        )(mark)
        at = 0
        for k in members:
            end = at + panels * widths[k] + LANES * (k == 0)
            held.append(gather(str(k), jnp.concatenate([x[:, at:end] for x in came], axis=0)))
            at = end

    depth = held_all[0].shape[0] + held[0][0].shape[0]
    core = lax.rem(lax.axis_index("panel"), EXP_DEV)
    if panel_width % LANES:
        by_core = [jnp.concatenate(x, axis=0) for x in zip(held_all, held[0])]
        both = jnp.stack([jnp.where(core == 0, *by_core), jnp.where(core == 0, *by_core[::-1])])
        rows = both[:, :, :width]
        scaled = (both[:, :, width : width + 1].astype(jnp.float32) * rows.astype(jnp.float32)).astype(jnp.bfloat16)
        mine = lax.dynamic_slice_in_dim(rows, lax.axis_index("panel") * panel_width, panel_width, 2)
        return jnp.einsum("eku,ekd->eud", mine, scaled, preferred_element_type=jnp.float32) * scaling

    out_type = jax.ShapeDtypeStruct((EXP_DEV, panel_width, width), jnp.float32)
    factor_type = jax.ShapeDtypeStruct((depth, LANES), jnp.bfloat16)
    anywhere = pl.BlockSpec(memory_space=pl.ANY)
    out = None
    factors = [None, None]
    old_scaled, old_panel = ([], []), ([], [])
    for k, members in enumerate(STEPS):
        w = sum(widths[j] for j in members)
        before = sum(widths[: members[0]])
        last = k == len(STEPS) - 1
        for side in range(EXP_DEV):
            final = int(last and side == EXP_DEV - 1)
            args = [held_all[side], *(held[j][side] for j in members), *old_scaled[side], *old_panel[side]]
            if k:
                args.append(factors[side])
            if final:
                args.append(mark)
            specs = [vmem] * len(args)
            if out is not None:
                args.append(out)
                specs.append(anywhere)
            outs = [out_type] if k else [out_type, factor_type]
            kept = [((depth, panels * w), jnp.bfloat16), ((w, depth), jnp.bfloat16)]
            scratch = [
                pltpu.VMEM((SLOTS, before + w, w), jnp.float32),
                pltpu.VMEM((SLOTS if k else 1, w, max(before, LANES)), jnp.float32),
                pltpu.SemaphoreType.DMA((2, SLOTS)),
            ]
            if last:
                scratch = [pltpu.VMEM(*x) for x in kept] + scratch
            else:
                outs += [jax.ShapeDtypeStruct(*x) for x in kept]
            flops = 2 * depth * panels * ((before + w) ** 2 - before**2)
            call = pl.pallas_call(
                functools.partial(hessian_kernel, k, side, final, widths, panels, scaling),
                out_shape=outs,
                in_specs=specs,
                out_specs=[anywhere] + [vmem] * (len(outs) - 1),
                scratch_shapes=scratch,
                input_output_aliases={} if out is None else {len(args) - 1: 0},
                compiler_params=pltpu.CompilerParams(vmem_limit_bytes=MAX_VMEM),
                cost_estimate=pl.CostEstimate(flops=flops, bytes_accessed=2 * flops // depth, transcendentals=0),
            )
            got = call(*args)
            out = got[0]
            if not k:
                factors[side] = got[1]
            if not last:
                old_scaled[side].append(got[-2])
                old_panel[side].append(got[-1])
    return out


def solution(mesh):
    placed = P(("expert", "panel"), None)

    return jax.shard_map(
        per_device,
        mesh=mesh,
        in_specs=(placed,) * 3,
        out_specs=P("expert", "panel", None),
        check_vma=False,
    )
```
